32 devices in a mesh: clip: 2 (over x), seq: 16 (over z, y, core).
Axes of the slice: x: 2, y: 2, z: 4, core: 2. Of those that a mesh axis runs over, the one named last changes fastest.
Arguments:
- hidden: bfloat16 [2, 1792, 1536], P(None, ('clip', 'seq')), parts along dimension 1, may hold values from -6 to 6
- latent: float32 [1792, 100], P(('clip', 'seq')), parts along dimension 0, may hold values from -6 to 6
- lengths: int32 [2], P('clip'), parts along dimension 0, may hold values from 448 to 896
- step_index: int32 [1], replicated, may hold values from 0 to 31
- guidance: float32 [1], replicated, may hold values from 1.5 to 2.5
- modulation: float32 [5, 1536], replicated, may hold values from -2.5 to 2.5
- conv_kernel: float32 [31, 1536], replicated, may hold values from -1 to 1
- w_qkv: bfloat16 [1536, 3072], replicated, may hold values from -1 to 1
- w_out: bfloat16 [1024, 1536], replicated, may hold values from -0.1875 to 0.1875
- w_mel: bfloat16 [1536, 100], replicated, may hold values from -0.15625 to 0.15625
Outputs:
- velocity: float32 [1792, 100], P(('clip', 'seq')), parts along dimension 0
- estimate: float32 [1792, 100], P(('clip', 'seq')), parts along dimension 0
The draws below stay inside these ranges and needn't reach their ends.
There are 2 independent parts, one for each index of `clip`. The reference program is written for one: setup_inputs(seed, part) draws one part's arguments, and reference() takes and returns one part's arrays. A program takes and returns all parts, laid end to end along the dimension named above; an argument that names none is the same for every part. Nothing has to cross between parts.
All inputs are finite; a program needn't handle non-finite values.
Results may differ from the reference program's by a relative error of at most 0.0061.
Values may be sent and summed in bfloat16 or wider, within the bound.
A program may use at most 192 MiB of HBM per device.

```python
import math
import jax
import jax.numpy as jnp
from jax import lax

D = 1536
HEADS = 16
HEAD_DIM = 64
MEL = 100
KERNEL = 31
STEPS = 32
HW = 1024
FRAMES = 896


def draw_w_qkv(key, part):
    attn_width = HEADS * HEAD_DIM
    columns = 3 * attn_width
    column_index = jnp.arange(columns)
    sharpen = jnp.where(column_index < 2 * attn_width, 2.0, 1.0)
    entries = jax.random.truncated_normal(jax.random.fold_in(key, 13), -4.0, 4.0, (D, columns), jnp.float32) * D ** (-0.5)
    entries = jnp.clip(entries * sharpen[None, :], -1.0, 1.0)
    return entries.astype(jnp.bfloat16)


def level_of(own_key, shape, shards, least, top_value):
    gain, own = 1.0, jax.random.fold_in(own_key, 6)
    for axis_at, shards_of in shards:
        steps = jnp.exp(jax.random.uniform(jax.random.fold_in(own, axis_at), (shards_of,), jnp.float32, least / len(shards), top_value / len(shards)))
        gain = gain * jnp.repeat(steps, shape[axis_at] // shards_of).reshape([-1 if axis == axis_at else 1 for axis in range(len(shape))])
    return gain


def normal_values(key, shape, deviation, most, split=(), kind=jnp.bfloat16):
    result = jax.random.normal(key, shape, jnp.float32) * deviation
    if len(split) > 0:
        result = level_of(key, shape, split, -0.22, 0.18) * result
    return jnp.clip(result, min=-most, max=most).astype(kind)


def setup_inputs(seed: int = 0, part: int = 0) -> dict:
    arg_keys = jax.random.split(jax.random.key(seed), 11)
    part_keys = jax.random.split(jax.random.fold_in(arg_keys[10], part), 11)
    return {
        "hidden": normal_values(part_keys[0], (2, FRAMES, D), 1.0, 6.0, ((1, 16),)),
        "latent": normal_values(part_keys[1], (FRAMES, MEL), 1.0, 6.0, ((0, 16),), jnp.float32),
        "lengths": jax.random.randint(part_keys[2], (1,), FRAMES // 2, FRAMES + 1).astype(jnp.int32),
        "step_index": jax.random.randint(arg_keys[3], (1,), 0, STEPS).astype(jnp.int32),
        "guidance": jnp.clip(jax.random.uniform(arg_keys[4], (1,), jnp.float32, 1.5, 2.5), 1.5, 2.5),
        "modulation": normal_values(arg_keys[5], (5, D), 0.5, 2.5, (), jnp.float32),
        "conv_kernel": normal_values(arg_keys[6], (KERNEL, D), KERNEL ** -0.5, 1.0, (), jnp.float32),
        "w_qkv": draw_w_qkv(jax.random.fold_in(arg_keys[10], 71), part),
        "w_out": normal_values(arg_keys[8], (HW, D), HW ** -0.5, 0.1875),
        "w_mel": normal_values(arg_keys[9], (D, MEL), D ** -0.5, 0.15625),
    }


EPSILON = 1e-06
NEGATIVE = -1e+30

def layer_norm(values, shift_row, scale_row):
    mean_value = lax.optimization_barrier(jnp.mean(values, axis=-1, keepdims=True))
    centered = values - mean_value
    variance = lax.optimization_barrier(jnp.mean(centered * centered, axis=-1, keepdims=True))
    return centered * lax.rsqrt(variance + EPSILON) * (1.0 + scale_row) + shift_row

def mish(values):
    return values * jnp.tanh(jax.nn.softplus(values))

def rotate(values, positions):
    half_dim = values.shape[-1] // 2
    inverse = 10000.0 ** (-jnp.arange(half_dim, dtype=jnp.float32) / half_dim)
    angles = positions.astype(jnp.float32)[:, None] * inverse[None, :]
    cosine = jnp.cos(angles)[:, None, :]
    sine_table = jnp.sin(angles)[:, None, :]
    lower_half = values[..., :half_dim]
    upper_half = values[..., half_dim:]
    return jnp.concatenate([lower_half * cosine - upper_half * sine_table, upper_half * cosine + lower_half * sine_table], axis=-1)

def reference(hidden, latent, lengths, step_index, guidance, modulation, conv_kernel, w_qkv, w_out, w_mel):
    positions = jnp.arange(FRAMES, dtype=jnp.int32)
    is_live = positions < lengths[0]
    masked = hidden * is_live[None, :, None].astype(jnp.bfloat16)
    half_width = KERNEL // 2
    padded = jnp.pad(masked, ((0, 0), (half_width, half_width), (0, 0)))
    convolved = jnp.zeros(hidden.shape, jnp.float32)
    for tap_index in range(KERNEL):
        convolved = convolved + conv_kernel[tap_index] * padded[:, tap_index:tap_index + FRAMES, :].astype(jnp.float32)
    residual = hidden.astype(jnp.float32) + mish(convolved)
    normed = layer_norm(residual, modulation[0], modulation[1]).astype(jnp.bfloat16)
    projected = jnp.dot(normed.reshape(-1, D), w_qkv, preferred_element_type=jnp.float32)
    projected = projected.reshape(2, FRAMES, 3, HEADS, HEAD_DIM)
    queries = rotate(projected[:, :, 0], positions).astype(jnp.bfloat16)
    keys_all = rotate(projected[:, :, 1], positions).astype(jnp.bfloat16).astype(jnp.float32)
    values_all = projected[:, :, 2].astype(jnp.bfloat16).astype(jnp.float32)
    block_rows = math.gcd(FRAMES, 512)
    query_blocks = queries.reshape(2, FRAMES // block_rows, block_rows, HEADS, HEAD_DIM).transpose(1, 0, 2, 3, 4)
    scale_factor = HEAD_DIM ** (-0.5)

    def attend_block(query_block):
        scores = jnp.einsum('cqhd,ckhd->chqk', query_block.astype(jnp.float32), keys_all) * scale_factor
        key_live = is_live[None, None, None, :]
        scores = jnp.where(key_live, scores, NEGATIVE)
        row_peak = lax.optimization_barrier(jnp.max(scores, axis=-1, keepdims=True))
        weights = jnp.where(key_live, jnp.exp(scores - row_peak), 0.0)
        weight_sum = lax.optimization_barrier(jnp.sum(weights, axis=-1))
        rounded = lax.optimization_barrier(weights.astype(jnp.bfloat16))
        weighted = jnp.einsum('chqk,ckhd->chqd', rounded.astype(jnp.float32), values_all)
        return (weighted / weight_sum[..., None]).transpose(0, 2, 1, 3).astype(jnp.bfloat16)
    attended = lax.map(attend_block, query_blocks)
    attended = attended.transpose(1, 0, 2, 3, 4).reshape(2 * FRAMES, HW)
    branch = jnp.dot(attended, w_out, preferred_element_type=jnp.float32).reshape(2, FRAMES, D)
    after = residual + modulation[2] * branch
    final_norm = layer_norm(after, modulation[3], modulation[4]).astype(jnp.bfloat16)
    speed = jnp.dot(final_norm.reshape(-1, D), w_mel, preferred_element_type=jnp.float32).reshape(2, FRAMES, MEL)
    guided = speed[0] + guidance[0] * (speed[0] - speed[1])
    velocity = jnp.where(is_live[:, None], guided, 0.0)
    progress = step_index[0].astype(jnp.float32) / STEPS
    time_now = 1.0 - jnp.cos(0.5 * jnp.pi * progress)
    estimate = latent + (1.0 - time_now) * velocity
    return (velocity, estimate)
```

```python
import functools

import jax
import jax.numpy as jnp
import numpy as np
from jax import lax
from jax.experimental import pallas as pl
from jax.experimental.pallas import tpu as pltpu
from jax.sharding import PartitionSpec as P

HEADS = 16
HEAD_DIM = 64
STEPS = 32
LANES = 128
EPSILON = 1e-06
NEGATIVE = -1e30
MESH = pl.DeviceIdType.MESH
ROW_BLOCK = 16
GROUPS = 4
BLOCKS = 2
PIECES = 2


def layer_norm(values, shift_row, scale_row):
    mean_value = jnp.mean(values, axis=-1, keepdims=True)
    centered = values - mean_value
    variance = jnp.mean(centered * centered, axis=-1, keepdims=True)
    return centered * lax.rsqrt(variance + EPSILON) * (1.0 + scale_row) + shift_row


def mish(values):
    grown = jnp.exp(jnp.minimum(values, 30.0))
    top = grown * (grown + 2.0)
    return values * (top / (top + 2.0))


def kernel(
    count,
    subs,
    frame_rows,
    taps,
    scalars,
    hidden_hbm,
    latent_hbm,
    modulation_hbm,
    conv_hbm,
    qkv_hbm,
    out_hbm,
    mel_hbm,
    row_table_hbm,
    base_table_hbm,
    velocity_ref,
    estimate_ref,
    hid,
    latent,
    halo,
    modulation,
    conv,
    w_qkv,
    w_out,
    w_mel,
    row_table,
    base_table,
    tables,
    residual,
    normed,
    q_send,
    kv_send,
    q_recv,
    kv_recv,
    o_send,
    o_recv,
    bias,
    local_sem,
    qkv_sem,
    halo_send_sem,
    halo_recv_sem,
    q_send_sem,
    q_recv_sem,
    kv_send_sem,
    kv_recv_sem,
    o_send_sem,
    o_recv_sem,
):
    copies = hid.shape[0]
    padded = hid.shape[1]
    reach = halo.shape[2]
    width = hid.shape[2]
    units = q_send.shape[0]
    per_group = units // GROUPS
    attention_width = w_out.shape[0]
    me = lax.axis_index("seq")
    own_rows = pl.ds(0, frame_rows)

    pulls = [
        (hidden_hbm, hid.at[:, pl.ds(0, frame_rows), :]),
        (conv_hbm, conv),
        (modulation_hbm, modulation),
        (row_table_hbm, row_table),
        (base_table_hbm.at[me], base_table),
        (latent_hbm, latent),
    ]
    local = [
        pltpu.make_async_copy(source, target, local_sem.at[i])
        for i, (source, target) in enumerate(pulls)
    ]
    for copy in local:
        copy.start()

    barrier = pltpu.get_barrier_semaphore()

    def greet(step, carry):
        pl.semaphore_signal(
            barrier, inc=1, device_id={"seq": (me + step) % count}, device_id_type=MESH
        )
        return carry

    lax.fori_loop(1, count, greet, 0)
    chunks = qkv_sem.shape[0]
    depth = width // chunks
    weights = [
        pltpu.make_async_copy(
            qkv_hbm.at[pl.ds(i * depth, depth)], w_qkv.at[pl.ds(i * depth, depth)], qkv_sem.at[i]
        )
        for i in range(chunks)
    ]
    late = [
        pltpu.make_async_copy(out_hbm, w_out, local_sem.at[len(pulls)]),
        pltpu.make_async_copy(mel_hbm, w_mel, local_sem.at[len(pulls) + 1]),
    ]
    for copy in weights + late:
        copy.start()
    hid[:, pl.ds(frame_rows, padded - frame_rows), :] = jnp.zeros(
        (copies, padded - frame_rows, width), hid.dtype
    )
    spare = pl.ds(frame_rows, padded - frame_rows)
    for buffer in (q_recv, o_recv):
        buffer[:, spare, :] = jnp.zeros((units, padded - frame_rows, LANES), buffer.dtype)
    kv_recv[:, :, spare, :] = jnp.zeros((count, 2, padded - frame_rows, LANES), kv_recv.dtype)

    pl.semaphore_wait(barrier, count - 1)
    piece_width = width // PIECES

    def halo_copies(c, piece):
        columns = pl.ds(piece * piece_width, piece_width)
        slot = c * PIECES + piece
        to_right = pltpu.make_async_remote_copy(
            src_ref=hidden_hbm.at[c, pl.ds(frame_rows - reach, reach), columns],
            dst_ref=halo.at[0, c, :, columns],
            send_sem=halo_send_sem.at[0, slot],
            recv_sem=halo_recv_sem.at[0, slot],
            device_id={"seq": (me + 1) % count},
            device_id_type=MESH,
        )
        to_left = pltpu.make_async_remote_copy(
            src_ref=hidden_hbm.at[c, pl.ds(0, reach), columns],
            dst_ref=halo.at[1, c, :, columns],
            send_sem=halo_send_sem.at[1, slot],
            recv_sem=halo_recv_sem.at[1, slot],
            device_id={"seq": (me + count - 1) % count},
            device_id_type=MESH,
        )
        return to_right, to_left

    halos = [halo_copies(c, piece) for c in range(copies) for piece in range(PIECES)]

    @pl.when(me < count - 1)
    def _():
        for to_right, _ in halos:
            to_right.start()

    @pl.when(me > 0)
    def _():
        for _, to_left in halos:
            to_left.start()

    @pl.when(me == 0)
    def _():
        halo[0] = jnp.zeros(halo.shape[1:], halo.dtype)

    @pl.when(me == count - 1)
    def _():
        halo[1] = jnp.zeros(halo.shape[1:], halo.dtype)

    for copy in local:
        copy.wait()
    length = scalars[0:1, :].astype(jnp.int32)

    base_cos = base_table[0:1, :]
    base_sin = base_table[1:2, :]
    row_cos = row_table[0]
    row_sin = row_table[1]
    lane = lax.broadcasted_iota(jnp.int32, (padded, LANES), 1)
    lower = lane % HEAD_DIM < HEAD_DIM // 2
    tables[0] = row_cos * base_cos - row_sin * base_sin
    sine = row_sin * base_cos + row_cos * base_sin
    tables[1] = jnp.where(lower, -sine, sine)
    key_index = lax.broadcasted_iota(jnp.int32, bias.shape, 1)
    key_row = key_index % padded
    key_position = (key_index // padded) * frame_rows + key_row
    key_live = (key_row < frame_rows) & (key_position < length[:, 0:1])
    bias[...] = jnp.where(key_live, 0.0, NEGATIVE)

    window = frame_rows + 2 * reach
    position = (
        me * frame_rows - reach + lax.broadcasted_iota(jnp.int32, (window, LANES), 0)
    )
    is_live = (position >= 0) & (position < length)
    lead = reach - taps // 2

    def convolve(c):
        def one(block, carry):
            columns = pl.ds(pl.multiple_of(block * LANES, LANES), LANES)
            own = hid[c, :, columns].astype(jnp.float32)
            cells = jnp.concatenate(
                [
                    halo[0, c, :, columns].astype(jnp.float32),
                    own[:frame_rows],
                    halo[1, c, :, columns].astype(jnp.float32),
                ],
                axis=0,
            )
            cells = jnp.where(is_live, cells, 0.0)
            total = jnp.zeros((padded, LANES), jnp.float32)
            for shift in range(8):
                part = None
                for first in range(0, reach * 2, 8):
                    tap = first + shift - lead
                    if 0 <= tap < taps:
                        term = cells[first : first + padded] * conv[pl.ds(tap, 1), columns]
                        part = term if part is None else part + term
                if part is not None:
                    total = total + (pltpu.roll(part, padded - shift, 0) if shift else part)
            residual[pl.ds(c * padded, padded), columns] = own + mish(total)
            return carry

        return one

    def convolve_copy(c):
        blocks = piece_width // LANES
        for piece in range(PIECES):
            to_right, to_left = halos[c * PIECES + piece]

            @pl.when(me < count - 1)
            def _():
                to_left.wait_recv()

            @pl.when(me > 0)
            def _():
                to_right.wait_recv()

            lax.fori_loop(piece * blocks, (piece + 1) * blocks, convolve(c), 0)

    def normalise(first, start, stop):
        for row in range(start, stop, ROW_BLOCK):
            rows = pl.ds(row, ROW_BLOCK)
            normed[rows, :] = layer_norm(
                residual[rows, :], modulation[first : first + 1, :], modulation[first + 1 : first + 2, :]
            ).astype(normed.dtype)

    my_group = me * GROUPS // count
    my_high = my_group // 2
    my_low = my_group % 2

    def group_at(step):
        return ((my_high + (3 - step) // 2) % 2) * 2 + (my_low + (step + 1) // 2) % 2

    my_unit = me // subs
    my_sub = me % subs
    query_sub = me // units
    query_slot = me % units

    def query_copy(unit):
        return pltpu.make_async_remote_copy(
            src_ref=q_send.at[unit, own_rows],
            dst_ref=q_recv.at[query_slot, own_rows],
            send_sem=q_send_sem.at[unit],
            recv_sem=q_recv_sem.at[query_slot],
            device_id={"seq": unit * subs + query_sub},
            device_id_type=MESH,
        )

    def key_value_copy(unit, sub):
        return pltpu.make_async_remote_copy(
            src_ref=kv_send.at[unit, :, own_rows],
            dst_ref=kv_recv.at[me, :, own_rows],
            send_sem=kv_send_sem.at[unit * subs + sub],
            recv_sem=kv_recv_sem.at[me],
            device_id={"seq": unit * subs + sub},
            device_id_type=MESH,
        )

    pair_width = 2 * LANES

    def rotate(tile, factor):
        half = HEAD_DIM // 2
        other = jnp.where(lower, pltpu.roll(tile, LANES - half, 1), pltpu.roll(tile, half, 1))
        return (tile * tables[0] + other * tables[1]) * factor

    def product(part, group, start, stop):
        first = pl.multiple_of(part * attention_width + group * pair_width, pair_width)
        return jnp.dot(
            normed[start:stop, :],
            w_qkv[:, pl.ds(first, pair_width)],
            preferred_element_type=jnp.float32,
        )

    def project_keys(c):
        def one(step, carry):
            group = group_at(step)
            key_pair = product(1, group, c * padded, (c + 1) * padded)
            value_pair = product(2, group, c * padded, (c + 1) * padded)
            for j in range(2):
                lanes = slice(j * LANES, (j + 1) * LANES)
                unit = group * per_group + j * copies + c
                kv_send[unit, 0] = rotate(key_pair[:, lanes], 1.0).astype(kv_send.dtype)
                kv_send[unit, 1] = value_pair[:, lanes].astype(kv_send.dtype)
            for j in range(2):
                unit = group * per_group + j * copies + c
                for sub in range(subs):

                    @pl.when(unit * subs + sub != me)
                    def _():
                        key_value_copy(unit, sub).start()

                    @pl.when(unit * subs + sub == me)
                    def _():
                        kv_recv[me, :, own_rows] = kv_send[unit, :, own_rows]

            return carry

        return one

    def project_queries(step, carry):
        group = group_at(step)
        query_pair = product(0, group, 0, copies * padded)
        for j in range(2):
            lanes = slice(j * LANES, (j + 1) * LANES)
            for c in range(copies):
                q_send[group * per_group + j * copies + c] = rotate(
                    query_pair[c * padded : (c + 1) * padded, lanes], HEAD_DIM**-0.5
                ).astype(q_send.dtype)

        def push(inner, carry):
            unit = group * per_group + inner

            @pl.when(unit * subs + query_sub != me)
            def _():
                query_copy(unit).start()

            @pl.when(unit * subs + query_sub == me)
            def _():
                q_recv[query_slot, own_rows] = q_send[unit, own_rows]

            return carry

        lax.fori_loop(0, per_group, push, 0)
        return carry

    for c in range(copies):
        convolve_copy(c)
        normalise(0, c * padded, (c + 1) * padded)
        if c == 0:
            for copy in weights:
                copy.wait()
        lax.fori_loop(0, GROUPS, project_keys(c), 0)
    lax.fori_loop(0, GROUPS, project_queries, 0)

    def arrived(block, semaphores, slot, source):
        pltpu.make_async_remote_copy(
            src_ref=block,
            dst_ref=block,
            send_sem=semaphores.at[slot],
            recv_sem=semaphores.at[slot],
            device_id={"seq": source},
            device_id_type=MESH,
        ).wait_recv()

    def wait_keys(source, carry):
        @pl.when(source != me)
        def _():
            arrived(kv_recv.at[source, :, own_rows], kv_recv_sem, source, source)

        return carry

    lax.fori_loop(0, count, wait_keys, 0)

    def returned(slot):
        return pltpu.make_async_remote_copy(
            src_ref=o_send.at[slot, own_rows],
            dst_ref=o_recv.at[my_unit, own_rows],
            send_sem=o_send_sem.at[slot],
            recv_sem=o_recv_sem.at[my_unit],
            device_id={"seq": my_sub * units + slot},
            device_id_type=MESH,
        )

    first_head = lane < HEAD_DIM
    keys_total = count * padded
    rounds = per_group // BLOCKS

    def attend(step, carry):
        pair = step // (2 * rounds)
        inner = step % (2 * rounds)
        group = ((my_high + inner % 2) % 2) * 2 + (my_low + pair) % 2
        base = group * per_group + (inner // 2) * BLOCKS
        for i in range(BLOCKS):
            source = my_sub * units + base + i

            @pl.when(source != me)
            def _():
                arrived(q_recv.at[base + i, own_rows], q_recv_sem, base + i, source)

        queries = [q_recv[base + i] for i in range(BLOCKS)]
        nothing = jnp.zeros_like(queries[0])
        both = jnp.concatenate(
            [jnp.where(first_head, query, nothing) for query in queries]
            + [jnp.where(first_head, nothing, query) for query in queries],
            axis=0,
        )
        keys = kv_recv[:, 0].reshape(keys_total, LANES)
        values = kv_recv[:, 1].reshape(keys_total, LANES)
        scores = lax.dot_general(
            both, keys, (((1,), (1,)), ((), ())), preferred_element_type=jnp.float32
        )
        scores = scores + bias[0:1, :]
        peak = jnp.max(scores, axis=-1, keepdims=True)
        exponentials = jnp.exp(scores - peak)
        weight_sum = jnp.sum(exponentials, axis=-1, keepdims=True)
        weighted = jnp.dot(
            exponentials.astype(values.dtype), values, preferred_element_type=jnp.float32
        )
        weighted = weighted / weight_sum
        half = BLOCKS * padded
        for i in range(BLOCKS):
            slot = base + i
            rows = slice(i * padded, (i + 1) * padded)
            o_send[slot] = jnp.where(first_head, weighted[:half][rows], weighted[half:][rows]).astype(
                o_send.dtype
            )

            @pl.when(my_sub * units + slot != me)
            def _():
                returned(slot).start()

            @pl.when(my_sub * units + slot == me)
            def _():
                o_recv[my_unit, own_rows] = o_send[slot, own_rows]

        return carry

    lax.fori_loop(0, units // BLOCKS, attend, 0)

    def sent(unit, carry):
        @pl.when(unit * subs + query_sub != me)
        def _():
            query_copy(unit).wait_send()

        for sub in range(subs):

            @pl.when(unit * subs + sub != me)
            def _():
                key_value_copy(unit, sub).wait_send()

        return carry

    lax.fori_loop(0, units, sent, 0)

    @pl.when(me < count - 1)
    def _():
        for to_right, _ in halos:
            to_right.wait_send()

    @pl.when(me > 0)
    def _():
        for _, to_left in halos:
            to_left.wait_send()

    for copy in late:
        copy.wait()

    def merge(step, carry):
        group = ((my_high + step % 2) % 2) * 2 + (my_low + step // 2) % 2
        for inner in range(per_group):
            unit = group * per_group + inner

            @pl.when(unit * subs + query_sub != me)
            def _():
                arrived(o_recv.at[unit, own_rows], o_recv_sem, unit, unit * subs + query_sub)

        attended = jnp.concatenate(
            [
                jnp.concatenate(
                    [o_recv[group * per_group + j * copies + c] for j in range(2)], axis=1
                )
                for c in range(copies)
            ],
            axis=0,
        )
        depth_rows = pl.ds(pl.multiple_of(group * pair_width, pair_width), pair_width)
        for first in range(0, width, pair_width):
            columns = slice(first, first + pair_width)
            branch = jnp.dot(attended, w_out[depth_rows, columns], preferred_element_type=jnp.float32)
            residual[:, columns] = residual[:, columns] + modulation[2:3, columns] * branch
        return carry

    lax.fori_loop(0, GROUPS, merge, 0)
    normalise(3, 0, copies * padded)
    speed = lax.dot_general(
        normed[...], w_mel[...], (((1,), (1,)), ((), ())), preferred_element_type=jnp.float32
    )
    speed_first = speed[:frame_rows]
    speed_second = speed[padded : padded + frame_rows]
    mel = speed.shape[1]
    guided = speed_first + scalars[2:3, :mel] * (speed_first - speed_second)
    own_position = me * frame_rows + lax.broadcasted_iota(jnp.int32, guided.shape, 0)
    velocity = jnp.where(own_position < length[:, :mel], guided, 0.0)
    progress = scalars[1:2, :mel] / STEPS
    time_now = 1.0 - jnp.cos(0.5 * jnp.pi * progress)
    velocity_ref[...] = velocity
    estimate_ref[...] = latent[...] + (1.0 - time_now) * velocity

    def finish(slot, carry):
        @pl.when(my_sub * units + slot != me)
        def _():
            returned(slot).wait_send()

        return carry

    lax.fori_loop(0, units, finish, 0)


def rotary_tables(padded, count, frame_rows):
    half = HEAD_DIM // 2
    inverse = 10000.0 ** (-(np.arange(LANES) % half) / half)
    rows = np.arange(padded)[:, None] * inverse[None, :]
    bases = (np.arange(count) * frame_rows)[:, None] * inverse[None, :]
    row_table = np.stack([np.cos(rows), np.sin(rows)]).astype(np.float32)
    base_table = np.stack([np.cos(bases), np.sin(bases)], axis=1).astype(np.float32)
    return row_table, base_table


def per_device(
    hidden, latent, lengths, step_index, guidance, modulation, conv_kernel, w_qkv, w_out, w_mel
):
    copies, frame_rows, width = hidden.shape
    taps = conv_kernel.shape[0]
    mel = w_mel.shape[1]
    count = lax.axis_size("seq")
    units = copies * HEADS * HEAD_DIM // LANES
    subs = count // units
    assert subs * units == count
    padded = -(-frame_rows // 16) * 16
    reach = -(-(taps // 2 + 1) // 8) * 8
    row_table, base_table = rotary_tables(padded, count, frame_rows)
    bf16 = jnp.bfloat16
    f32 = jnp.float32
    dma = pltpu.SemaphoreType.DMA
    scalars = jnp.concatenate(
        [
            jnp.broadcast_to(value.astype(f32)[:, None], (1, LANES))
            for value in (lengths, step_index, guidance)
        ]
    )
    return pl.pallas_call(
        functools.partial(kernel, count, subs, frame_rows, taps),
        out_shape=[pltpu.VMEM((frame_rows, mel), f32)] * 2,
        in_specs=[pl.BlockSpec(memory_space=pltpu.VMEM)] + [pl.BlockSpec(memory_space=pl.ANY)] * 9,
        out_specs=[pl.BlockSpec(memory_space=pltpu.VMEM)] * 2,
        scratch_shapes=[
            pltpu.VMEM((copies, padded, width), bf16),
            pltpu.VMEM((frame_rows, mel), f32),
            pltpu.VMEM((2, copies, reach, width), bf16),
            pltpu.VMEM(modulation.shape, f32),
            pltpu.VMEM(conv_kernel.shape, f32),
            pltpu.VMEM(w_qkv.shape, bf16),
            pltpu.VMEM(w_out.shape, bf16),
            pltpu.VMEM((mel, width), bf16),
            pltpu.VMEM(row_table.shape, f32),
            pltpu.VMEM(base_table.shape[1:], f32),
            pltpu.VMEM((2, padded, LANES), f32),
            pltpu.VMEM((copies * padded, width), f32),
            pltpu.VMEM((copies * padded, width), bf16),
            pltpu.VMEM((units, padded, LANES), bf16),
            pltpu.VMEM((units, 2, padded, LANES), bf16),
            pltpu.VMEM((units, padded, LANES), bf16),
            pltpu.VMEM((count, 2, padded, LANES), bf16),
            pltpu.VMEM((units, padded, LANES), bf16),
            pltpu.VMEM((units, padded, LANES), bf16),
            pltpu.VMEM((8, count * padded), f32),
            dma((8,)),
            dma((6,)),
            dma((2, copies * PIECES)),
            dma((2, copies * PIECES)),
            dma((units,)),
            dma((units,)),
            dma((count,)),
            dma((count,)),
            dma((units,)),
            dma((units,)),
        ],
        compiler_params=pltpu.CompilerParams(
            collective_id=0, has_side_effects=True, vmem_limit_bytes=40 * 1024 * 1024
        ),
    )(
        pltpu.with_memory_space_constraint(scalars, pltpu.VMEM),
        *(
            pltpu.with_memory_space_constraint(operand, pltpu.HBM)
            for operand in (
                hidden,
                latent,
                modulation,
                conv_kernel,
                w_qkv,
                w_out,
                w_mel.T,
                jnp.asarray(row_table),
                jnp.asarray(base_table),
            )
        )
    )


def solution(mesh):
    return jax.shard_map(
        per_device,
        mesh=mesh,
        in_specs=(
            P(None, ("clip", "seq"), None),
            P(("clip", "seq"), None),
            P("clip"),
            P(),
            P(),
            P(),
            P(),
            P(),
            P(),
            P(),
        ),
        out_specs=(P(("clip", "seq"), None), P(("clip", "seq"), None)),
        check_vma=False,
    )
```

```python
import functools

import jax
import jax.numpy as jnp
import numpy as np
from jax import lax
from jax.experimental import pallas as pl
from jax.experimental.pallas import tpu as pltpu
from jax.sharding import PartitionSpec as P

HEADS = 16
HEAD_DIM = 64
STEPS = 32
LANES = 128
EPSILON = 1e-06
NEGATIVE = -1e30
MESH = pl.DeviceIdType.MESH
ROW_BLOCK = 16
GROUPS = 4
BLOCKS = 2
PIECES = 2


def layer_norm(values, shift_row, scale_row):
    mean_value = jnp.mean(values, axis=-1, keepdims=True)
    centered = values - mean_value
    variance = jnp.mean(centered * centered, axis=-1, keepdims=True)
    return centered * lax.rsqrt(variance + EPSILON) * (1.0 + scale_row) + shift_row


def mish(values):
    grown = jnp.exp(jnp.minimum(values, 30.0))
    top = grown * (grown + 2.0)
    return values * (top / (top + 2.0))


def kernel(
    count,
    subs,
    frame_rows,
    taps,
    scalars,
    hidden_hbm,
    latent_hbm,
    modulation_hbm,
    conv_hbm,
    qkv_hbm,
    out_hbm,
    mel_hbm,
    row_table_hbm,
    base_table_hbm,
    velocity_ref,
    estimate_ref,
    hid,
    latent,
    halo,
    modulation,
    conv,
    w_qkv,
    w_out,
    w_mel,
    row_table,
    base_table,
    tables,
    residual,
    normed,
    q_send,
    kv_send,
    q_recv,
    kv_recv,
    o_send,
    o_recv,
    bias,
    local_sem,
    qkv_sem,
    halo_send_sem,
    halo_recv_sem,
    q_send_sem,
    q_recv_sem,
    kv_send_sem,
    kv_recv_sem,
    o_send_sem,
    o_recv_sem,
    from_below,
    from_above,
):
    copies = hid.shape[0]
    padded = hid.shape[1]
    reach = halo.shape[2]
    width = hid.shape[2]
    units = q_send.shape[0]
    per_group = units // GROUPS
    attention_width = w_out.shape[0]
    me = lax.axis_index("seq")
    own_rows = pl.ds(0, frame_rows)

    pulls = [
        (hidden_hbm, hid.at[:, pl.ds(0, frame_rows), :]),
        (conv_hbm, conv),
        (modulation_hbm, modulation),
        (row_table_hbm, row_table),
        (base_table_hbm.at[me], base_table),
        (latent_hbm, latent),
    ]
    local = [
        pltpu.make_async_copy(source, target, local_sem.at[i])
        for i, (source, target) in enumerate(pulls)
    ]
    for copy in local:
        copy.start()

    barrier = pltpu.get_barrier_semaphore()

    def signal(semaphore, target):
        pl.semaphore_signal(semaphore, inc=1, device_id={"seq": target}, device_id_type=MESH)

    plane = count // GROUPS
    my_group = me // plane
    my_place = me % plane
    below = my_group > 0
    above = my_group < GROUPS - 1
    first_place = my_place == 0
    last_place = my_place == plane - 1

    def greet(step, carry):
        signal(barrier, my_group * plane + (my_place + step) % plane)
        return carry

    @pl.when(below)
    def _():
        signal(barrier, me - plane)

    @pl.when(above)
    def _():
        signal(barrier, me + plane)

    @pl.when(below & first_place)
    def _():
        signal(barrier, me - 1)

    @pl.when(above & last_place)
    def _():
        signal(barrier, me + 1)

    lax.fori_loop(1, plane, greet, 0)
    my_high = my_group // 2
    my_low = my_group % 2

    def group_at(step):
        return ((my_high + (3 - step) // 2) % 2) * 2 + (my_low + (step + 1) // 2) % 2

    pair_width = 2 * LANES

    def weight_columns(part, group):
        return pl.ds(
            pl.multiple_of(part * attention_width + group * pair_width, pair_width), pair_width
        )

    def weight_copy(part, step):
        columns = weight_columns(part, group_at(step))
        return pltpu.make_async_copy(
            qkv_hbm.at[:, columns], w_qkv.at[:, columns], qkv_sem.at[part, step]
        )

    late = [
        pltpu.make_async_copy(out_hbm, w_out, local_sem.at[len(pulls)]),
        pltpu.make_async_copy(mel_hbm, w_mel, local_sem.at[len(pulls) + 1]),
    ]
    for step in range(GROUPS):
        weight_copy(1, step).start()
        weight_copy(2, step).start()
    for step in range(GROUPS):
        weight_copy(0, step).start()
    for copy in late:
        copy.start()
    hid[:, pl.ds(frame_rows, padded - frame_rows), :] = jnp.zeros(
        (copies, padded - frame_rows, width), hid.dtype
    )
    spare = pl.ds(frame_rows, padded - frame_rows)
    for buffer in (q_recv, o_recv):
        buffer[:, spare, :] = jnp.zeros((units, padded - frame_rows, LANES), buffer.dtype)
    kv_recv[:, :, spare, :] = jnp.zeros((count, 2, padded - frame_rows, LANES), kv_recv.dtype)

    sides = below.astype(jnp.int32) + above.astype(jnp.int32)
    corners = (below & first_place).astype(jnp.int32) + (above & last_place).astype(jnp.int32)
    pl.semaphore_wait(barrier, plane - 1 + sides + corners)

    @pl.when(above)
    def _():
        signal(from_below.at[0], me + plane)

    @pl.when(below)
    def _():
        signal(from_above.at[0], me - plane)

    def relay(hop):
        @pl.when(my_group >= hop)
        def _():
            pl.semaphore_wait(from_below.at[hop - 1], 1)

        @pl.when(GROUPS - 1 - my_group >= hop)
        def _():
            pl.semaphore_wait(from_above.at[hop - 1], 1)

        if hop < GROUPS - 1:

            @pl.when((my_group >= hop) & above)
            def _():
                signal(from_below.at[hop], me + plane)

            @pl.when((GROUPS - 1 - my_group >= hop) & below)
            def _():
                signal(from_above.at[hop], me - plane)

    piece_width = width // PIECES

    def halo_copies(c, piece):
        columns = pl.ds(piece * piece_width, piece_width)
        slot = c * PIECES + piece
        to_right = pltpu.make_async_remote_copy(
            src_ref=hidden_hbm.at[c, pl.ds(frame_rows - reach, reach), columns],
            dst_ref=halo.at[0, c, :, columns],
            send_sem=halo_send_sem.at[0, slot],
            recv_sem=halo_recv_sem.at[0, slot],
            device_id={"seq": (me + 1) % count},
            device_id_type=MESH,
        )
        to_left = pltpu.make_async_remote_copy(
            src_ref=hidden_hbm.at[c, pl.ds(0, reach), columns],
            dst_ref=halo.at[1, c, :, columns],
            send_sem=halo_send_sem.at[1, slot],
            recv_sem=halo_recv_sem.at[1, slot],
            device_id={"seq": (me + count - 1) % count},
            device_id_type=MESH,
        )
        return to_right, to_left

    halos = [halo_copies(c, piece) for c in range(copies) for piece in range(PIECES)]

    @pl.when(me < count - 1)
    def _():
        for to_right, _ in halos:
            to_right.start()

    @pl.when(me > 0)
    def _():
        for _, to_left in halos:
            to_left.start()

    @pl.when(me == 0)
    def _():
        halo[0] = jnp.zeros(halo.shape[1:], halo.dtype)

    @pl.when(me == count - 1)
    def _():
        halo[1] = jnp.zeros(halo.shape[1:], halo.dtype)

    relay(1)
    for copy in local:
        copy.wait()
    length = scalars[0:1, :].astype(jnp.int32)

    base_cos = base_table[0:1, :]
    base_sin = base_table[1:2, :]
    row_cos = row_table[0]
    row_sin = row_table[1]
    lane = lax.broadcasted_iota(jnp.int32, (padded, LANES), 1)
    lower = lane % HEAD_DIM < HEAD_DIM // 2
    tables[0] = row_cos * base_cos - row_sin * base_sin
    sine = row_sin * base_cos + row_cos * base_sin
    tables[1] = jnp.where(lower, -sine, sine)
    key_index = lax.broadcasted_iota(jnp.int32, bias.shape, 1)
    key_row = key_index % padded
    key_position = (key_index // padded) * frame_rows + key_row
    key_live = (key_row < frame_rows) & (key_position < length[:, 0:1])
    bias[...] = jnp.where(key_live, 0.0, NEGATIVE)

    own_position = me * frame_rows + lax.broadcasted_iota(jnp.int32, (frame_rows, LANES), 0)
    own_live = own_position < length
    row16 = lax.broadcasted_iota(jnp.int32, (reach, LANES), 0)
    right_live = (me + 1) * frame_rows + row16 < length
    left_live = me * frame_rows - reach + row16 < length
    lead = reach - taps // 2
    spare_rows = padded - frame_rows
    tail = reach + spare_rows

    def shifted(part, shift):
        return pltpu.roll(part, part.shape[0] - shift, 0) if shift else part

    def gather(groups, shift, columns, pieces):
        part = None
        for first in groups:
            tap = first + shift - lead
            if 0 <= tap < taps:
                term = pieces(first) * conv[pl.ds(tap, 1), columns]
                part = term if part is None else part + term
        return part

    def convolve_own(c):
        def one(block, carry):
            columns = pl.ds(pl.multiple_of(block * LANES, LANES), LANES)
            own = jnp.where(own_live, hid[c, :frame_rows, columns].astype(jnp.float32), 0.0)
            blank = jnp.zeros((reach, LANES), jnp.float32)
            cells = jnp.concatenate([blank, own, blank], axis=0)
            total = None
            for shift in range(8):
                part = gather(
                    range(0, reach * 2, 8), shift, columns, lambda first: cells[first : first + padded]
                )
                part = shifted(part, shift)
                total = part if total is None else total + part
            residual[pl.ds(c * padded, padded), columns] = total
            return carry

        lax.fori_loop(0, width // LANES, one, 0)

    def convolve_edges(c):
        def one(block, carry):
            columns = pl.ds(pl.multiple_of(block * LANES, LANES), LANES)
            left = jnp.where(left_live, halo[0, c, :, columns].astype(jnp.float32), 0.0)
            right = jnp.where(right_live, halo[1, c, :, columns].astype(jnp.float32), 0.0)
            blank = jnp.zeros((reach, LANES), jnp.float32)
            left_cells = jnp.concatenate([left, blank], axis=0)
            right_cells = jnp.concatenate([blank, right], axis=0)
            left_total = None
            right_total = None
            for shift in range(8):
                part = gather(
                    range(0, reach, 8), shift, columns, lambda first: left_cells[first : first + reach]
                )
                if part is not None:
                    part = shifted(jnp.where(row16 < shift, 0.0, part) if shift else part, shift)
                    left_total = part if left_total is None else left_total + part
                part = gather(
                    range(reach, reach * 2, 8),
                    shift,
                    columns,
                    lambda first: right_cells[first - reach : first - reach + tail],
                )
                if part is not None:
                    part = shifted(part, shift)
                    right_total = part if right_total is None else right_total + part
            own = hid[c, :, columns].astype(jnp.float32)
            base = c * padded
            for first, stop in ((0, reach), (reach, padded - tail), (padded - tail, padded)):
                rows = pl.ds(base + first, stop - first)
                total = residual[rows, columns]
                if first == 0:
                    total = total + left_total
                if stop == padded:
                    total = total + right_total
                residual[rows, columns] = own[first:stop] + mish(total)
            return carry

        blocks = piece_width // LANES
        for piece in range(PIECES):
            to_right, to_left = halos[c * PIECES + piece]

            @pl.when(me < count - 1)
            def _():
                to_left.wait_recv()

            @pl.when(me > 0)
            def _():
                to_right.wait_recv()

            lax.fori_loop(piece * blocks, (piece + 1) * blocks, one, 0)

    def normalise(first, start, stop):
        for row in range(start, stop, ROW_BLOCK):
            rows = pl.ds(row, ROW_BLOCK)
            normed[rows, :] = layer_norm(
                residual[rows, :], modulation[first : first + 1, :], modulation[first + 1 : first + 2, :]
            ).astype(normed.dtype)

    my_unit = me // subs
    my_sub = me % subs
    query_sub = me // units
    query_slot = me % units

    def query_copy(unit):
        return pltpu.make_async_remote_copy(
            src_ref=q_send.at[unit, own_rows],
            dst_ref=q_recv.at[query_slot, own_rows],
            send_sem=q_send_sem.at[unit],
            recv_sem=q_recv_sem.at[query_slot],
            device_id={"seq": unit * subs + query_sub},
            device_id_type=MESH,
        )

    def key_value_copy(unit, sub):
        return pltpu.make_async_remote_copy(
            src_ref=kv_send.at[unit, :, own_rows],
            dst_ref=kv_recv.at[me, :, own_rows],
            send_sem=kv_send_sem.at[unit * subs + sub],
            recv_sem=kv_recv_sem.at[me],
            device_id={"seq": unit * subs + sub},
            device_id_type=MESH,
        )

    def rotate(tile, factor):
        half = HEAD_DIM // 2
        other = jnp.where(lower, pltpu.roll(tile, LANES - half, 1), pltpu.roll(tile, half, 1))
        return (tile * tables[0] + other * tables[1]) * factor

    def product(part, group, start, stop):
        return jnp.dot(
            normed[start:stop, :],
            w_qkv[:, weight_columns(part, group)],
            preferred_element_type=jnp.float32,
        )

    def project_keys(c):
        def one(step, carry):
            group = group_at(step)
            if c == 0:
                weight_copy(1, step).wait()
                weight_copy(2, step).wait()
            key_pair = product(1, group, c * padded, (c + 1) * padded)
            value_pair = product(2, group, c * padded, (c + 1) * padded)
            for j in range(2):
                lanes = slice(j * LANES, (j + 1) * LANES)
                unit = group * per_group + j * copies + c
                kv_send[unit, 0] = rotate(key_pair[:, lanes], 1.0).astype(kv_send.dtype)
                kv_send[unit, 1] = value_pair[:, lanes].astype(kv_send.dtype)
            for j in range(2):
                unit = group * per_group + j * copies + c
                for sub in range(subs):

                    @pl.when(unit * subs + sub != me)
                    def _():
                        key_value_copy(unit, sub).start()

                    @pl.when(unit * subs + sub == me)
                    def _():
                        kv_recv[me, :, own_rows] = kv_send[unit, :, own_rows]

            return carry

        return one

    def project_queries(step, carry):
        group = group_at(step)
        weight_copy(0, step).wait()
        query_pair = product(0, group, 0, copies * padded)
        for j in range(2):
            lanes = slice(j * LANES, (j + 1) * LANES)
            for c in range(copies):
                q_send[group * per_group + j * copies + c] = rotate(
                    query_pair[c * padded : (c + 1) * padded, lanes], HEAD_DIM**-0.5
                ).astype(q_send.dtype)

        def push(inner, carry):
            unit = group * per_group + inner

            @pl.when(unit * subs + query_sub != me)
            def _():
                query_copy(unit).start()

            @pl.when(unit * subs + query_sub == me)
            def _():
                q_recv[query_slot, own_rows] = q_send[unit, own_rows]

            return carry

        lax.fori_loop(0, per_group, push, 0)
        return carry

    convolve_own(0)
    for hop in range(2, GROUPS - 1):
        relay(hop)
    for c in range(copies):
        if c:
            convolve_own(c)
        convolve_edges(c)
        normalise(0, c * padded, (c + 1) * padded)
        if c == 0:
            relay(GROUPS - 1)
        lax.fori_loop(0, GROUPS, project_keys(c), 0)
    lax.fori_loop(0, GROUPS, project_queries, 0)

    def arrived(block, semaphores, slot, source):
        pltpu.make_async_remote_copy(
            src_ref=block,
            dst_ref=block,
            send_sem=semaphores.at[slot],
            recv_sem=semaphores.at[slot],
            device_id={"seq": source},
            device_id_type=MESH,
        ).wait_recv()

    def wait_keys(source, carry):
        @pl.when(source != me)
        def _():
            arrived(kv_recv.at[source, :, own_rows], kv_recv_sem, source, source)

        return carry

    lax.fori_loop(0, count, wait_keys, 0)

    def returned(slot):
        return pltpu.make_async_remote_copy(
            src_ref=o_send.at[slot, own_rows],
            dst_ref=o_recv.at[my_unit, own_rows],
            send_sem=o_send_sem.at[slot],
            recv_sem=o_recv_sem.at[my_unit],
            device_id={"seq": my_sub * units + slot},
            device_id_type=MESH,
        )

    first_head = lane < HEAD_DIM
    keys_total = count * padded
    rounds = per_group // BLOCKS

    def attend(step, carry):
        pair = step // (2 * rounds)
        inner = step % (2 * rounds)
        group = ((my_high + inner % 2) % 2) * 2 + (my_low + pair) % 2
        base = group * per_group + (inner // 2) * BLOCKS
        for i in range(BLOCKS):
            source = my_sub * units + base + i

            @pl.when(source != me)
            def _():
                arrived(q_recv.at[base + i, own_rows], q_recv_sem, base + i, source)

        queries = [q_recv[base + i] for i in range(BLOCKS)]
        nothing = jnp.zeros_like(queries[0])
        both = jnp.concatenate(
            [jnp.where(first_head, query, nothing) for query in queries]
            + [jnp.where(first_head, nothing, query) for query in queries],
            axis=0,
        )
        keys = kv_recv[:, 0].reshape(keys_total, LANES)
        values = kv_recv[:, 1].reshape(keys_total, LANES)
        scores = lax.dot_general(
            both, keys, (((1,), (1,)), ((), ())), preferred_element_type=jnp.float32
        )
        scores = scores + bias[0:1, :]
        peak = jnp.max(scores, axis=-1, keepdims=True)
        exponentials = jnp.exp(scores - peak)
        weight_sum = jnp.sum(exponentials, axis=-1, keepdims=True)
        weighted = jnp.dot(
            exponentials.astype(values.dtype), values, preferred_element_type=jnp.float32
        )
        weighted = weighted / weight_sum
        half = BLOCKS * padded
        for i in range(BLOCKS):
            slot = base + i
            rows = slice(i * padded, (i + 1) * padded)
            o_send[slot] = jnp.where(first_head, weighted[:half][rows], weighted[half:][rows]).astype(
                o_send.dtype
            )

            @pl.when(my_sub * units + slot != me)
            def _():
                returned(slot).start()

            @pl.when(my_sub * units + slot == me)
            def _():
                o_recv[my_unit, own_rows] = o_send[slot, own_rows]

        return carry

    lax.fori_loop(0, units // BLOCKS, attend, 0)

    def sent(unit, carry):
        @pl.when(unit * subs + query_sub != me)
        def _():
            query_copy(unit).wait_send()

        for sub in range(subs):

            @pl.when(unit * subs + sub != me)
            def _():
                key_value_copy(unit, sub).wait_send()

        return carry

    lax.fori_loop(0, units, sent, 0)

    @pl.when(me < count - 1)
    def _():
        for to_right, _ in halos:
            to_right.wait_send()

    @pl.when(me > 0)
    def _():
        for _, to_left in halos:
            to_left.wait_send()

    for copy in late:
        copy.wait()

    def merge(step, carry):
        group = ((my_high + step % 2) % 2) * 2 + (my_low + step // 2) % 2
        for inner in range(per_group):
            unit = group * per_group + inner

            @pl.when(unit * subs + query_sub != me)
            def _():
                arrived(o_recv.at[unit, own_rows], o_recv_sem, unit, unit * subs + query_sub)

        attended = jnp.concatenate(
            [
                jnp.concatenate(
                    [o_recv[group * per_group + j * copies + c] for j in range(2)], axis=1
                )
                for c in range(copies)
            ],
            axis=0,
        )
        depth_rows = pl.ds(pl.multiple_of(group * pair_width, pair_width), pair_width)
        for first in range(0, width, pair_width):
            columns = slice(first, first + pair_width)
            branch = jnp.dot(attended, w_out[depth_rows, columns], preferred_element_type=jnp.float32)
            residual[:, columns] = residual[:, columns] + modulation[2:3, columns] * branch
        return carry

    lax.fori_loop(0, GROUPS, merge, 0)
    normalise(3, 0, copies * padded)
    speed = lax.dot_general(
        normed[...], w_mel[...], (((1,), (1,)), ((), ())), preferred_element_type=jnp.float32
    )
    speed_first = speed[:frame_rows]
    speed_second = speed[padded : padded + frame_rows]
    mel = speed.shape[1]
    guided = speed_first + scalars[2:3, :mel] * (speed_first - speed_second)
    row_position = me * frame_rows + lax.broadcasted_iota(jnp.int32, guided.shape, 0)
    velocity = jnp.where(row_position < length[:, :mel], guided, 0.0)
    progress = scalars[1:2, :mel] / STEPS
    time_now = 1.0 - jnp.cos(0.5 * jnp.pi * progress)
    velocity_ref[...] = velocity
    estimate_ref[...] = latent[...] + (1.0 - time_now) * velocity

    def finish(slot, carry):
        @pl.when(my_sub * units + slot != me)
        def _():
            returned(slot).wait_send()

        return carry

    lax.fori_loop(0, units, finish, 0)


def rotary_tables(padded, count, frame_rows):
    half = HEAD_DIM // 2
    inverse = 10000.0 ** (-(np.arange(LANES) % half) / half)
    rows = np.arange(padded)[:, None] * inverse[None, :]
    bases = (np.arange(count) * frame_rows)[:, None] * inverse[None, :]
    row_table = np.stack([np.cos(rows), np.sin(rows)]).astype(np.float32)
    base_table = np.stack([np.cos(bases), np.sin(bases)], axis=1).astype(np.float32)
    return row_table, base_table


def per_device(
    hidden, latent, lengths, step_index, guidance, modulation, conv_kernel, w_qkv, w_out, w_mel
):
    copies, frame_rows, width = hidden.shape
    taps = conv_kernel.shape[0]
    mel = w_mel.shape[1]
    count = lax.axis_size("seq")
    units = copies * HEADS * HEAD_DIM // LANES
    subs = count // units
    assert subs * units == count
    padded = -(-frame_rows // 16) * 16
    reach = -(-(taps // 2 + 1) // 8) * 8
    row_table, base_table = rotary_tables(padded, count, frame_rows)
    bf16 = jnp.bfloat16
    f32 = jnp.float32
    dma = pltpu.SemaphoreType.DMA
    scalars = jnp.concatenate(
        [
            jnp.broadcast_to(value.astype(f32)[:, None], (1, LANES))
            for value in (lengths, step_index, guidance)
        ]
    )
    return pl.pallas_call(
        functools.partial(kernel, count, subs, frame_rows, taps),
        out_shape=[pltpu.VMEM((frame_rows, mel), f32)] * 2,
        in_specs=[pl.BlockSpec(memory_space=pltpu.VMEM)] + [pl.BlockSpec(memory_space=pl.ANY)] * 9,
        out_specs=[pl.BlockSpec(memory_space=pltpu.VMEM)] * 2,
        scratch_shapes=[
            pltpu.VMEM((copies, padded, width), bf16),
            pltpu.VMEM((frame_rows, mel), f32),
            pltpu.VMEM((2, copies, reach, width), bf16),
            pltpu.VMEM(modulation.shape, f32),
            pltpu.VMEM(conv_kernel.shape, f32),
            pltpu.VMEM(w_qkv.shape, bf16),
            pltpu.VMEM(w_out.shape, bf16),
            pltpu.VMEM((mel, width), bf16),
            pltpu.VMEM(row_table.shape, f32),
            pltpu.VMEM(base_table.shape[1:], f32),
            pltpu.VMEM((2, padded, LANES), f32),
            pltpu.VMEM((copies * padded, width), f32),
            pltpu.VMEM((copies * padded, width), bf16),
            pltpu.VMEM((units, padded, LANES), bf16),
            pltpu.VMEM((units, 2, padded, LANES), bf16),
            pltpu.VMEM((units, padded, LANES), bf16),
            pltpu.VMEM((count, 2, padded, LANES), bf16),
            pltpu.VMEM((units, padded, LANES), bf16),
            pltpu.VMEM((units, padded, LANES), bf16),
            pltpu.VMEM((8, count * padded), f32),
            dma((8,)),
            dma((3, GROUPS)),
            dma((2, copies * PIECES)),
            dma((2, copies * PIECES)),
            dma((units,)),
            dma((units,)),
            dma((count,)),
            dma((count,)),
            dma((units,)),
            dma((units,)),
            pltpu.SemaphoreType.REGULAR((GROUPS - 1,)),
            pltpu.SemaphoreType.REGULAR((GROUPS - 1,)),
        ],
        compiler_params=pltpu.CompilerParams(
            collective_id=0, has_side_effects=True, vmem_limit_bytes=40 * 1024 * 1024
        ),
    )(
        pltpu.with_memory_space_constraint(scalars, pltpu.VMEM),
        *(
            pltpu.with_memory_space_constraint(operand, pltpu.HBM)
            for operand in (
                hidden,
                latent,
                modulation,
                conv_kernel,
                w_qkv,
                w_out,
                w_mel.T,
                jnp.asarray(row_table),
                jnp.asarray(base_table),
            )
        )
    )


def solution(mesh):
    return jax.shard_map(
        per_device,
        mesh=mesh,
        in_specs=(
            P(None, ("clip", "seq"), None),
            P(("clip", "seq"), None),
            P("clip"),
            P(),
            P(),
            P(),
            P(),
            P(),
            P(),
            P(),
        ),
        out_specs=(P(("clip", "seq"), None), P(("clip", "seq"), None)),
        check_vma=False,
    )
```
